32 devices in a mesh: gx: 4 (over y, core), gy: 4 (over z), gz: 2 (over x).
Axes of the slice: x: 2, y: 2, z: 4, core: 2. Of those that a mesh axis runs over, the one named last changes fastest.
Arguments:
- order_param: float32 [16, 64, 256], P('gx', 'gy', 'gz'), may hold values from -1 to 1
- density: float32 [16, 64, 256], P('gx', 'gy', 'gz'), may hold values from 0.7 to 1.3
- velocity: float32 [3, 16, 64, 256], P(None, 'gx', 'gy', 'gz'), may hold values from -0.3 to 0.3
Outputs:
- final_order: float32 [16, 64, 256], P('gx', 'gy', 'gz')
- populations: float32 [19, 16, 64, 256], P(None, 'gx', 'gy', 'gz')
The draws below stay inside these ranges and needn't reach their ends.
All inputs are finite; a program needn't handle non-finite values.
Results may differ from the reference program's by a relative error of at most 0.0001.
Values sent between devices are 32-bit elements; how exact they have to be, the bound alone decides.
A program may use at most 64 MiB of HBM per device.

```python
import jax
import jax.numpy as jnp

ITERS = 5
NX = 16
NY = 64
NZ = 256


def block_scale(rng, extent, shards, smallest, top_value):
    factor_of, own = 1.0, jax.random.fold_in(rng, 6)
    for dim, shards_of in shards:
        draws = jnp.exp(jax.random.uniform(jax.random.fold_in(own, dim), (shards_of,), jnp.float32, smallest / len(shards), top_value / len(shards)))
        factor_of = factor_of * jnp.repeat(draws, extent[dim] // shards_of).reshape([-1 if axis == dim else 1 for axis in range(len(extent))])
    return factor_of


def bell_draw(rng, shape, deviation, reach, split=(), held_as=jnp.bfloat16):
    entries = jax.random.normal(rng, shape, jnp.float32) * deviation
    if len(split) > 0:
        entries = block_scale(rng, shape, split, -0.22, 0.18) * entries
    return jnp.clip(entries, min=-reach, max=reach).astype(held_as)


def setup_inputs(seed: int = 0) -> dict:
    seeds = jax.random.split(jax.random.key(seed), 4)
    return {
        "order_param": jnp.clip(jax.random.uniform(seeds[0], (NX, NY, NZ), jnp.float32, -1.0, 1.0) * block_scale(seeds[0], (NX, NY, NZ), ((0, 4), (1, 4), (2, 2)), -0.4, 0.0), -1.0, 1.0),
        "density": jnp.clip(0.7 + 0.59999996 * jax.random.uniform(seeds[1], (NX, NY, NZ), jnp.float32) ** block_scale(seeds[1], (NX, NY, NZ), ((0, 4), (1, 4), (2, 2)), -0.2, 0.2), 0.7, 1.3),
        "velocity": bell_draw(seeds[2], (3, NX, NY, NZ), 0.1, 0.3, ((1, 4), (2, 4), (3, 2)), jnp.float32),
    }


DIRECTIONS = [(0, 0, 0), (1, 0, 0), (-1, 0, 0), (0, 1, 0), (0, -1, 0), (0, 0, 1), (0, 0, -1),
              (1, 1, 0), (-1, -1, 0), (1, -1, 0), (-1, 1, 0), (1, 0, 1), (-1, 0, -1), (1, 0, -1),
              (-1, 0, 1), (0, 1, 1), (0, -1, -1), (0, 1, -1), (0, -1, 1)]
WEIGHTS = [1.0 / 3.0] + [1.0 / 18.0] * 6 + [1.0 / 36.0] * 12
quadratic = -0.1
quartic = 0.1
stiffness = 0.02
mobility = 0.5
relax_time = 0.8


def equilibrium(dens, flow):
    usq = flow[0] * flow[0] + flow[1] * flow[1] + flow[2] * flow[2]
    out = []
    for i in range(19):
        along = jnp.zeros_like(dens)
        for d in range(3):
            if DIRECTIONS[i][d] != 0:
                along = along + DIRECTIONS[i][d] * flow[d]
        out.append(WEIGHTS[i] * dens * (1.0 + 3.0 * along + 4.5 * along * along - 1.5 * usq))
    return jnp.stack(out)


def moments(pops):
    dens = jnp.sum(pops, axis=0)
    moms = []
    for d in range(3):
        total = jnp.zeros_like(dens)
        for i in range(19):
            if DIRECTIONS[i][d] == 1:
                total = total + pops[i]
            elif DIRECTIONS[i][d] == -1:
                total = total - pops[i]
        moms.append(total)
    return dens, jnp.stack(moms)


def reference(order_param, density, velocity):
    order = order_param
    pops = equilibrium(density, velocity)
    for step in range(ITERS):
        beside = -6.0 * order
        for d in range(3):
            beside = beside + jnp.roll(order, 1, d) + jnp.roll(order, -1, d)
        chem = quadratic * order + quartic * order * order * order - stiffness * beside
        force = jnp.stack([-order * (jnp.roll(chem, -1, d) - jnp.roll(chem, 1, d)) * 0.5 for d in range(3)])
        dens, moms = moments(pops)
        vel = moms / dens
        base = equilibrium(dens, vel)
        moved = equilibrium(dens, vel + force / dens)
        post = pops - (pops - base) / relax_time + moved - base
        pops = jnp.stack([jnp.roll(post[i], DIRECTIONS[i], (0, 1, 2)) for i in range(19)])
        dens2, moms2 = moments(pops)
        flow = moms2 / dens2
        change = jnp.zeros_like(order)
        for d in range(3):
            flux = 0.25 * (flow[d] + jnp.roll(flow[d], -1, d)) * (order + jnp.roll(order, -1, d)) - mobility * (jnp.roll(chem, -1, d) - chem)
            change = change + flux - jnp.roll(flux, 1, d)
        order = order - change
    return order, pops
```

```python
import functools

import jax
import jax.numpy as jnp
from jax import lax
from jax.experimental import pallas as pl
from jax.experimental.pallas import tpu as pltpu
from jax.sharding import PartitionSpec as P

ITERS = 5
MESH = pl.DeviceIdType.MESH
DIRS = [
    (0, 0, 0),
    (1, 0, 0),
    (-1, 0, 0),
    (0, 1, 0),
    (0, -1, 0),
    (0, 0, 1),
    (0, 0, -1),
    (1, 1, 0),
    (-1, -1, 0),
    (1, -1, 0),
    (-1, 1, 0),
    (1, 0, 1),
    (-1, 0, -1),
    (1, 0, -1),
    (-1, 0, 1),
    (0, 1, 1),
    (0, -1, -1),
    (0, 1, -1),
    (0, -1, 1),
]
WEIGHTS = [1.0 / 3.0] + [1.0 / 18.0] * 6 + [1.0 / 36.0] * 12
quadratic = -0.1
quartic = 0.1
stiffness = 0.02
mobility = 0.5
relax_time = 0.8

SIGNS = (1, -1)
INDEX = {1: 0, -1: 1}
CROSS = [{s: [i for i in range(19) if DIRS[i][d] == s] for s in SIGNS} for d in range(3)]
EDGES = [(a, b) for a in SIGNS for b in SIGNS]
LANES = 8


def neighbours():
    out = []
    for d in range(3):
        for s in SIGNS:
            out.append(tuple(s if k == d else 0 for k in range(3)))
    out += [(a, b, 0) for a, b in EDGES]
    out += [(a, 0, b) for a, b in EDGES]
    out += [(0, a, b) for a, b in EDGES]
    return out


def kernel(sizes, order_in, dens_in, vel_in, order, pops, post, *scratch):
    (ax, ay, az, rax, ray, raz, raxy, raxz, rayz) = scratch[0:9]
    (by, bz, rbx, rby, rbz, rbxy, rbxz, rbyzr, rbyzc) = scratch[9:18]
    (cx_, cy_, cz_, rcx, rcy, rcz) = scratch[18:24]
    (sa, ra, sb, rb, sc, rc) = scratch[24:30]
    X, Y, Z = order.shape
    me = [lax.axis_index(a) for a in ("gx", "gy", "gz")]

    def device(off):
        return {
            a: lax.rem(me[k] + (off[k] + sizes[k]), sizes[k]) if off[k] else me[k]
            for k, a in enumerate(("gx", "gy", "gz"))
        }

    barrier = pltpu.get_barrier_semaphore()
    for off in neighbours():
        pl.semaphore_signal(barrier, inc=1, device_id=device(off), device_id_type=MESH)

    lane = lax.broadcasted_iota(jnp.int32, (Y, Z), 1)
    row = lax.broadcasted_iota(jnp.int32, (Y, Z), 0)
    lane8 = lax.broadcasted_iota(jnp.int32, (8, Z), 1)
    row8 = lax.broadcasted_iota(jnp.int32, (8, Z), 0)
    lane1 = lax.broadcasted_iota(jnp.int32, (1, Z), 1)

    def roll(v, s, axis):
        s = s % v.shape[axis]
        return v if s == 0 else pltpu.roll(v, s, axis)

    def zend(s):
        return 0 if s == 1 else Z - 1

    def yend(s):
        return 0 if s == 1 else Y - 1

    def zshift(v, s, packed, at):
        col = roll(packed, zend(s) - at, 1)
        return jnp.where(lane == zend(s), col, roll(v, s, 1))

    def yshift(v, s, halo):
        return jnp.where(row == yend(s), jnp.broadcast_to(halo, v.shape), roll(v, s, 0))

    def rowshift(v, s, edge, lanes):
        return jnp.where(lanes == zend(s), roll(edge, s, 1), roll(v, s, 1))

    def pack(fields, s):
        acc = jnp.zeros((Y, Z), jnp.float32)
        for slot, planes in enumerate(fields):
            for x in range(X):
                at = slot * LANES + 1 + x
                depth_lane = planes[x][1]
                acc = jnp.where(lane == at, roll(planes[x][0], at - depth_lane, 1), acc)
        return acc

    def run(messages, ssem, rsem):
        copies = []
        for k, (src, dst, off) in enumerate(messages):
            copy = pltpu.make_async_remote_copy(
                src_ref=src,
                dst_ref=dst,
                send_sem=ssem.at[k],
                recv_sem=rsem.at[k],
                device_id=device(off),
                device_id_type=MESH,
            )
            copy.start()
            copies.append(copy)
        return copies

    def finish(copies):
        for copy in copies:
            copy.wait_recv()
        for copy in copies:
            copy.wait_send()

    for ref in (ay, by, cy_):
        ref[...] = jnp.zeros_like(ref)

    for x in range(X):
        order[x] = order_in[x]
        r = dens_in[x]
        u = [vel_in[d, x] for d in range(3)]
        usq = 1.0 - 1.5 * (u[0] * u[0] + u[1] * u[1] + u[2] * u[2])
        for i in range(19):
            along = None
            for d in range(3):
                if DIRS[i][d]:
                    t = u[d] if DIRS[i][d] == 1 else -u[d]
                    along = t if along is None else along + t
            if along is None:
                pops[i, x] = WEIGHTS[i] * r * usq
            else:
                pops[i, x] = WEIGHTS[i] * r * (usq + 3.0 * along + 4.5 * along * along)
    pl.semaphore_wait(barrier, len(neighbours()))

    def moments(ps):
        rho = ps[0]
        for i in range(1, 19):
            rho = rho + ps[i]
        moms = []
        for d in range(3):
            up = functools.reduce(lambda a, b: a + b, [ps[i] for i in CROSS[d][1]])
            down = functools.reduce(lambda a, b: a + b, [ps[i] for i in CROSS[d][-1]])
            moms.append(up - down)
        return rho, moms

    def chemical(o, beside):
        return quadratic * o + quartic * o * o * o - stiffness * (beside - 6.0 * o)

    def step(_, carry):
        O = [order[x] for x in range(X)]
        for s in SIGNS:
            si = INDEX[s]
            for depth in range(2):
                y = Y - 1 - depth if s == 1 else depth
                for x in range(X):
                    by[si, depth, 1 + x : 2 + x, :] = O[x][y : y + 1, :]
            bz[si] = pack(
                [
                    [(O[x], Z - 1 - depth if s == 1 else depth) for x in range(X)]
                    for depth in range(2)
                ],
                s,
            )
        messages = []
        for s in SIGNS:
            si = INDEX[s]
            planes = order.at[pl.ds(X - 2, 2)] if s == 1 else order.at[pl.ds(0, 2)]
            messages.append((planes, rbx.at[si], (s, 0, 0)))
            messages.append((by.at[si], rby.at[si], (0, s, 0)))
            messages.append((bz.at[si], rbz.at[si], (0, 0, s)))
        for e, (a, b) in enumerate(EDGES):
            messages.append((by.at[INDEX[b], 0], rbxy.at[e], (a, b, 0)))
            messages.append((bz.at[INDEX[b]], rbxz.at[e], (a, 0, b)))
            messages.append((by.at[INDEX[a], 0], rbyzr.at[e], (0, a, b)))
            half = bz.at[INDEX[b], pl.ds(Y - 8, 8)] if a == 1 else bz.at[INDEX[b], pl.ds(0, 8)]
            messages.append((half, rbyzc.at[e], (0, a, b)))
        finish(run(messages, sb, rb))

        edge = {ab: e for e, ab in enumerate(EDGES)}
        OX = {-2: rbx[0, 0], -1: rbx[0, 1], X: rbx[1, 0], X + 1: rbx[1, 1]}
        for x in range(X):
            OX[x] = O[x]

        def order_y(x, s):
            return yshift(O[x], s, rby[INDEX[s], 0, 1 + x : 2 + x, :])

        def order_z(x, s):
            return zshift(O[x], s, rbz[INDEX[s]], 1 + x)

        C, pairs = {}, []
        for x in range(X):
            near = {(0, 1): OX[x - 1], (0, -1): OX[x + 1]}
            for s in SIGNS:
                near[(1, s)], near[(2, s)] = order_y(x, s), order_z(x, s)
            C[x] = chemical(O[x], functools.reduce(lambda a, b: a + b, near.values()))
            pairs.append({k: O[x] + v for k, v in near.items()})
        for s in SIGNS:
            x = -1 if s == 1 else X
            far = X - 1 if s == 1 else 0
            p = OX[x]
            beside = OX[x - 1] + OX[x + 1]
            for t in SIGNS:
                e = edge[(s, t)]
                beside = beside + yshift(p, t, rbxy[e, 1 + far : 2 + far, :])
                beside = beside + zshift(p, t, rbxz[e], 1 + far)
            C[x] = chemical(p, beside)
        CY, CZ = {}, {}
        for s in SIGNS:
            near = rby[INDEX[s], 0]
            full = jnp.where(row8 == 0, roll(rbxy[edge[(1, s)]], -X, 0), near)
            full = jnp.where(row8 == X + 1, roll(rbxy[edge[(-1, s)]], X, 0), full)
            beside = rby[INDEX[s], 1] + by[INDEX[-s], 0] + roll(full, 1, 0) + roll(full, -1, 0)
            for t in SIGNS:
                beside = beside + rowshift(near, t, rbyzr[edge[(s, t)]], lane8)
            CY[s] = chemical(near, beside)

            near = rbz[INDEX[s]]
            full = jnp.where(lane == 0, roll(rbxz[edge[(1, s)]], -X, 1), near)
            full = jnp.where(lane == X + 1, roll(rbxz[edge[(-1, s)]], X, 1), full)
            beside = roll(near, -LANES, 1) + bz[INDEX[-s]] + roll(full, 1, 1) + roll(full, -1, 1)
            for t in SIGNS:
                k = 7 if t == 1 else 0
                beside = beside + yshift(near, t, rbyzc[edge[(t, s)], k : k + 1, :])
            CZ[s] = chemical(near, beside)

        diffused = []
        for x in range(X):
            c = C[x]
            cy_up = yshift(c, -1, CY[-1][1 + x : 2 + x, :])
            cy_dn = yshift(c, 1, CY[1][1 + x : 2 + x, :])
            cz_up = zshift(c, -1, CZ[-1], 1 + x)
            cz_dn = zshift(c, 1, CZ[1], 1 + x)
            diffused.append(
                C[x + 1] + C[x - 1] + cy_up + cy_dn + cz_up + cz_dn - 6.0 * c
            )
            scale = -0.5 * O[x]
            force = [scale * (C[x + 1] - C[x - 1]), scale * (cy_up - cy_dn), scale * (cz_up - cz_dn)]
            ps = [pops[i, x] for i in range(19)]
            rho, moms = moments(ps)
            inv = 1.0 / rho
            u = [m * inv for m in moms]
            v = [u[d] + force[d] * inv for d in range(3)]
            keep = 1.0 - 1.0 / relax_time
            mix = 1.0 / relax_time - 1.0
            usq = u[0] * u[0] + u[1] * u[1] + u[2] * u[2]
            vsq = v[0] * v[0] + v[1] * v[1] + v[2] * v[2]
            flat = rho * ((mix + 1.0) - 1.5 * (mix * usq + vsq))
            out = [None] * 19
            out[0] = keep * ps[0] + WEIGHTS[0] * flat
            for i in range(1, 19, 2):
                a, b = None, None
                for d in range(3):
                    if DIRS[i][d]:
                        tu = u[d] if DIRS[i][d] == 1 else -u[d]
                        tv = v[d] if DIRS[i][d] == 1 else -v[d]
                        a = tu if a is None else a + tu
                        b = tv if b is None else b + tv
                even = WEIGHTS[i] * flat + (4.5 * WEIGHTS[i]) * rho * (mix * a * a + b * b)
                odd = (3.0 * WEIGHTS[i]) * rho * (mix * a + b)
                out[i] = keep * ps[i] + even + odd
                out[i + 1] = keep * ps[i + 1] + even - odd
            for i in range(19):
                post[i, x] = out[i]
            for s in SIGNS:
                if x == (X - 1 if s == 1 else 0):
                    for slot, i in enumerate(CROSS[0][s]):
                        ax[INDEX[s], slot] = out[i]
                y = Y - 1 if s == 1 else 0
                for slot, i in enumerate(CROSS[1][s]):
                    ay[INDEX[s], slot, 1 + x : 2 + x, :] = out[i][y : y + 1, :]
        for s in SIGNS:
            az[INDEX[s]] = pack(
                [[(post[i, x], Z - 1 if s == 1 else 0) for x in range(X)] for i in CROSS[2][s]], s
            )

        messages = []
        for s in SIGNS:
            si = INDEX[s]
            messages.append((ax.at[si], rax.at[si], (s, 0, 0)))
            messages.append((ay.at[si], ray.at[si], (0, s, 0)))
            messages.append((az.at[si], raz.at[si], (0, 0, s)))
        for e, (a, b) in enumerate(EDGES):
            slot = CROSS[1][b].index(DIRS.index((a, b, 0)))
            messages.append((ay.at[INDEX[b], slot], raxy.at[e], (a, b, 0)))
            messages.append((az.at[INDEX[b]], raxz.at[e], (a, 0, b)))
            slot = CROSS[1][a].index(DIRS.index((0, a, b)))
            messages.append((ay.at[INDEX[a], slot], rayz.at[e], (0, a, b)))
        finish(run(messages, sa, ra))

        flows = []
        for x in range(X):
            ps = []
            for i, (cx, cy, cz) in enumerate(DIRS):
                xs = x - cx
                own = 0 <= xs < X
                far = X - 1 if cx == 1 else 0
                p = post[i, xs] if own else rax[INDEX[cx], CROSS[0][cx].index(i)]
                if cz:
                    at = CROSS[2][cz].index(i) * LANES + 1
                    if own:
                        p = zshift(p, cz, raz[INDEX[cz]], at + xs)
                    else:
                        p = zshift(p, cz, raxz[edge[(cx, cz)]], at + far)
                if cy:
                    if own:
                        halo = ray[INDEX[cy], CROSS[1][cy].index(i), 1 + xs : 2 + xs, :]
                    else:
                        halo = raxy[edge[(cx, cy)], 1 + far : 2 + far, :]
                    if cz:
                        halo = rowshift(halo, cz, rayz[edge[(cy, cz)], 1 + x : 2 + x, :], lane1)
                    p = yshift(p, cy, halo)
                pops[i, x] = p
                ps.append(p)
            rho, moms = moments(ps)
            inv = 1.0 / rho
            flows.append([m * inv for m in moms])

        for s in SIGNS:
            si = INDEX[s]
            y = Y - 1 if s == 1 else 0
            cx_[si] = flows[X - 1 if s == 1 else 0][0]
            for x in range(X):
                cy_[si, 1 + x : 2 + x, :] = flows[x][1][y : y + 1, :]
            cz_[si] = pack([[(flows[x][2], Z - 1 if s == 1 else 0) for x in range(X)]], s)
        messages = []
        for s in SIGNS:
            si = INDEX[s]
            messages.append((cx_.at[si], rcx.at[si], (s, 0, 0)))
            messages.append((cy_.at[si], rcy.at[si], (0, s, 0)))
            messages.append((cz_.at[si], rcz.at[si], (0, 0, s)))
        finish(run(messages, sc, rc))

        for x in range(X):
            f, pair = flows[x], pairs[x]
            fx_up = flows[x + 1][0] if x + 1 < X else rcx[1]
            fx_dn = flows[x - 1][0] if x > 0 else rcx[0]
            change = (f[0] + fx_up) * pair[(0, -1)] - (f[0] + fx_dn) * pair[(0, 1)]
            for s in SIGNS:
                fy = yshift(f[1], s, rcy[INDEX[s], 1 + x : 2 + x, :])
                fz = zshift(f[2], s, rcz[INDEX[s]], 1 + x)
                part = (f[1] + fy) * pair[(1, s)] + (f[2] + fz) * pair[(2, s)]
                change = change - part if s == 1 else change + part
            order[x] = O[x] - (0.25 * change - mobility * diffused[x])
        return carry

    lax.fori_loop(0, ITERS, step, 0)


def on_device(sizes, order_param, density, velocity):
    X, Y, Z = order_param.shape
    f32 = jnp.float32
    plane, rows = (Y, Z), (8, Z)
    vmem = [
        (19, X, Y, Z),
        (2, 5) + plane, (2, 5) + rows, (2,) + plane,
        (2, 5) + plane, (2, 5) + rows, (2,) + plane,
        (4,) + rows, (4,) + plane, (4,) + rows,
        (2, 2) + rows, (2,) + plane,
        (2, 2) + plane, (2, 2) + rows, (2,) + plane,
        (4,) + rows, (4,) + plane, (4,) + rows, (4,) + rows,
        (2,) + plane, (2,) + rows, (2,) + plane,
        (2,) + plane, (2,) + rows, (2,) + plane,
    ]
    sems = [18, 18, 22, 22, 6, 6]
    spec = pl.BlockSpec(memory_space=pltpu.VMEM)
    return pl.pallas_call(
        functools.partial(kernel, sizes),
        out_shape=(
            jax.ShapeDtypeStruct((X, Y, Z), f32),
            jax.ShapeDtypeStruct((19, X, Y, Z), f32),
        ),
        in_specs=[spec] * 3,
        out_specs=(spec, spec),
        scratch_shapes=[pltpu.VMEM(s, f32) for s in vmem]
        + [pltpu.SemaphoreType.DMA((n,)) for n in sems],
        compiler_params=pltpu.CompilerParams(collective_id=0, has_side_effects=True),
    )(order_param, density, velocity)


def solution(mesh):
    sizes = tuple(mesh.shape[a] for a in ("gx", "gy", "gz"))
    return jax.shard_map(
        functools.partial(on_device, sizes),
        mesh=mesh,
        in_specs=(P("gx", "gy", "gz"), P("gx", "gy", "gz"), P(None, "gx", "gy", "gz")),
        out_specs=(P("gx", "gy", "gz"), P(None, "gx", "gy", "gz")),
        check_vma=False,
    )
```

```python
import functools

import jax
import jax.numpy as jnp
from jax import lax
from jax.experimental import pallas as pl
from jax.experimental.pallas import tpu as pltpu
from jax.sharding import PartitionSpec as P

ITERS = 5
MESH = pl.DeviceIdType.MESH
DIRS = [
    (0, 0, 0),
    (1, 0, 0),
    (-1, 0, 0),
    (0, 1, 0),
    (0, -1, 0),
    (0, 0, 1),
    (0, 0, -1),
    (1, 1, 0),
    (-1, -1, 0),
    (1, -1, 0),
    (-1, 1, 0),
    (1, 0, 1),
    (-1, 0, -1),
    (1, 0, -1),
    (-1, 0, 1),
    (0, 1, 1),
    (0, -1, -1),
    (0, 1, -1),
    (0, -1, 1),
]
WEIGHTS = [1.0 / 3.0] + [1.0 / 18.0] * 6 + [1.0 / 36.0] * 12
quadratic = -0.1
quartic = 0.1
stiffness = 0.02
mobility = 0.5
relax_time = 0.8

SIGNS = (1, -1)
INDEX = {1: 0, -1: 1}
CROSS = [{s: [i for i in range(19) if DIRS[i][d] == s] for s in SIGNS} for d in range(3)]
EDGES = [(a, b) for a in SIGNS for b in SIGNS]
LANES = 8


def neighbours():
    out = []
    for d in range(3):
        for s in SIGNS:
            out.append(tuple(s if k == d else 0 for k in range(3)))
    out += [(a, b, 0) for a, b in EDGES]
    out += [(a, 0, b) for a, b in EDGES]
    out += [(0, a, b) for a, b in EDGES]
    return out


def kernel(sizes, order_in, dens_in, vel_in, order, pops, post, *scratch):
    (ax, ay, az, rax, ray, raz, ae, rae) = scratch[0:8]
    (by, bz, rbx, rby, rbz, be, rbe) = scratch[8:15]
    (cx_, cy_, cz_, rcx, rcy, rcz) = scratch[15:21]
    (sa, ra, sb, rb, sc, rc) = scratch[21:27]
    X, Y, Z = order.shape
    me = [lax.axis_index(a) for a in ("gx", "gy", "gz")]

    def device(off):
        return {
            a: lax.rem(me[k] + (off[k] + sizes[k]), sizes[k]) if off[k] else me[k]
            for k, a in enumerate(("gx", "gy", "gz"))
        }

    barrier = pltpu.get_barrier_semaphore()
    for off in neighbours():
        pl.semaphore_signal(barrier, inc=1, device_id=device(off), device_id_type=MESH)

    lane = lax.broadcasted_iota(jnp.int32, (Y, Z), 1)
    row = lax.broadcasted_iota(jnp.int32, (Y, Z), 0)
    lane8 = lax.broadcasted_iota(jnp.int32, (8, Z), 1)
    row8 = lax.broadcasted_iota(jnp.int32, (8, Z), 0)
    lane1 = lax.broadcasted_iota(jnp.int32, (1, Z), 1)

    def roll(v, s, axis):
        s = s % v.shape[axis]
        return v if s == 0 else pltpu.roll(v, s, axis)

    def zend(s):
        return 0 if s == 1 else Z - 1

    def yend(s):
        return 0 if s == 1 else Y - 1

    def zshift(v, s, packed, at):
        col = roll(packed, zend(s) - at, 1)
        return jnp.where(lane == zend(s), col, roll(v, s, 1))

    def yshift(v, s, halo):
        return jnp.where(row == yend(s), jnp.broadcast_to(halo, v.shape), roll(v, s, 0))

    def zinsert(v, s, col, lanes):
        return jnp.where(lanes == zend(s), jnp.broadcast_to(col, v.shape), roll(v, s, 1))

    def to_row(v, z):
        col = jnp.broadcast_to(v[:, z : z + 1], v.shape)
        return jnp.sum(jnp.where(lane == row, col, 0.0), axis=0, keepdims=True)

    def to_col(v, lanes, rows):
        v = jnp.broadcast_to(v, lanes.shape)
        return jnp.sum(jnp.where(lanes == rows, v, 0.0), axis=1, keepdims=True)

    def xsrc(s):
        return X - 1 if s == 1 else 0

    def ysrc(s):
        return Y - 1 if s == 1 else 0

    def zsrc(s):
        return Z - 1 if s == 1 else 0

    def corners(planes, b, c):
        y, acc = ysrc(b), jnp.zeros((1, Z), jnp.float32)
        for x in range(X):
            cells = roll(planes[x][y : y + 1, :], 1 + x - zsrc(c), 1)
            acc = jnp.where(lane1 == 1 + x, cells, acc)
        return acc

    def pack(fields, s):
        acc = jnp.zeros((Y, Z), jnp.float32)
        for slot, planes in enumerate(fields):
            for x in range(X):
                at = slot * LANES + 1 + x
                depth_lane = planes[x][1]
                acc = jnp.where(lane == at, roll(planes[x][0], at - depth_lane, 1), acc)
        return acc

    def run(messages, ssem, rsem):
        copies = []
        for k, (src, dst, off) in enumerate(messages):
            copy = pltpu.make_async_remote_copy(
                src_ref=src,
                dst_ref=dst,
                send_sem=ssem.at[k],
                recv_sem=rsem.at[k],
                device_id=device(off),
                device_id_type=MESH,
            )
            copy.start()
            copies.append(copy)
        return copies

    def finish(copies):
        for copy in copies:
            copy.wait_recv()
        for copy in copies:
            copy.wait_send()

    for ref in (ay, by, cy_):
        ref[...] = jnp.zeros_like(ref)

    for x in range(X):
        order[x] = order_in[x]
        r = dens_in[x]
        u = [vel_in[d, x] for d in range(3)]
        usq = 1.0 - 1.5 * (u[0] * u[0] + u[1] * u[1] + u[2] * u[2])
        for i in range(19):
            along = None
            for d in range(3):
                if DIRS[i][d]:
                    t = u[d] if DIRS[i][d] == 1 else -u[d]
                    along = t if along is None else along + t
            if along is None:
                pops[i, x] = WEIGHTS[i] * r * usq
            else:
                pops[i, x] = WEIGHTS[i] * r * (usq + 3.0 * along + 4.5 * along * along)
    pl.semaphore_wait(barrier, len(neighbours()))

    def moments(ps):
        rho = ps[0]
        for i in range(1, 19):
            rho = rho + ps[i]
        moms = []
        for d in range(3):
            up = functools.reduce(lambda a, b: a + b, [ps[i] for i in CROSS[d][1]])
            down = functools.reduce(lambda a, b: a + b, [ps[i] for i in CROSS[d][-1]])
            moms.append(up - down)
        return rho, moms

    def chemical(o, beside):
        return quadratic * o + quartic * o * o * o - stiffness * (beside - 6.0 * o)

    def step(_, carry):
        O = [order[x] for x in range(X)]
        for s in SIGNS:
            si = INDEX[s]
            for depth in range(2):
                y = Y - 1 - depth if s == 1 else depth
                for x in range(X):
                    by[si, depth, 1 + x : 2 + x, :] = O[x][y : y + 1, :]
            bz[si] = pack(
                [
                    [(O[x], Z - 1 - depth if s == 1 else depth) for x in range(X)]
                    for depth in range(2)
                ],
                s,
            )
        messages = []
        for s in SIGNS:
            si = INDEX[s]
            planes = order.at[pl.ds(X - 2, 2)] if s == 1 else order.at[pl.ds(0, 2)]
            messages.append((planes, rbx.at[si], (s, 0, 0)))
            messages.append((by.at[si], rby.at[si], (0, s, 0)))
            messages.append((bz.at[si], rbz.at[si], (0, 0, s)))
        for e, (a, b) in enumerate(EDGES):
            be[e] = O[xsrc(a)][ysrc(b) : ysrc(b) + 1, :]
            be[4 + e] = to_row(O[xsrc(a)], zsrc(b))
            be[8 + e] = corners(O, a, b)
            messages.append((be.at[e], rbe.at[e], (a, b, 0)))
            messages.append((be.at[4 + e], rbe.at[4 + e], (a, 0, b)))
            messages.append((be.at[8 + e], rbe.at[8 + e], (0, a, b)))
        flying = run(messages, sb, rb)

        keep = 1.0 - 1.0 / relax_time
        mix = 1.0 / relax_time - 1.0

        def along(i, w):
            a = None
            for d in range(3):
                if DIRS[i][d]:
                    t = w[d] if DIRS[i][d] == 1 else -w[d]
                    a = t if a is None else a + t
            return a

        moved = []
        for x in range(X):
            ps = [pops[i, x] for i in range(19)]
            rho, moms = moments(ps)
            inv = 1.0 / rho
            u = [m * inv for m in moms]
            flat = (mix * rho) * (1.0 - 1.5 * (u[0] * u[0] + u[1] * u[1] + u[2] * u[2]))
            post[0, x] = keep * ps[0] + WEIGHTS[0] * flat
            for i in range(1, 19, 2):
                a = along(i, u)
                even = WEIGHTS[i] * flat + (4.5 * mix * WEIGHTS[i]) * rho * (a * a)
                odd = (3.0 * mix * WEIGHTS[i]) * rho * a
                post[i, x] = keep * ps[i] + even + odd
                post[i + 1, x] = keep * ps[i + 1] + even - odd
            moved.append((rho, inv, u))
        finish(flying)

        edge = {ab: e for e, ab in enumerate(EDGES)}
        OX = {-2: rbx[0, 0], -1: rbx[0, 1], X: rbx[1, 0], X + 1: rbx[1, 1]}
        for x in range(X):
            OX[x] = O[x]

        def order_y(x, s):
            return yshift(O[x], s, rby[INDEX[s], 0, 1 + x : 2 + x, :])

        def order_z(x, s):
            return zshift(O[x], s, rbz[INDEX[s]], 1 + x)

        C, pairs = {}, []
        for x in range(X):
            near = {(0, 1): OX[x - 1], (0, -1): OX[x + 1]}
            for s in SIGNS:
                near[(1, s)], near[(2, s)] = order_y(x, s), order_z(x, s)
            C[x] = chemical(O[x], functools.reduce(lambda a, b: a + b, near.values()))
            pairs.append({k: O[x] + v for k, v in near.items()})
        for s in SIGNS:
            x = -1 if s == 1 else X
            p = OX[x]
            beside = OX[x - 1] + OX[x + 1]
            for t in SIGNS:
                e = edge[(s, t)]
                beside = beside + yshift(p, t, rbe[e])
                beside = beside + zinsert(p, t, to_col(rbe[4 + e], lane, row), lane)
            C[x] = chemical(p, beside)
        CY, CZ = {}, {}
        for s in SIGNS:
            near = rby[INDEX[s], 0]
            full = jnp.where(row8 == 0, jnp.broadcast_to(rbe[edge[(1, s)]], near.shape), near)
            after = jnp.broadcast_to(rbe[edge[(-1, s)]], near.shape)
            full = jnp.where(row8 == X + 1, after, full)
            beside = rby[INDEX[s], 1] + by[INDEX[-s], 0] + roll(full, 1, 0) + roll(full, -1, 0)
            for t in SIGNS:
                col = to_col(rbe[8 + edge[(s, t)]], lane8, row8)
                beside = beside + zinsert(near, t, col, lane8)
            CY[s] = chemical(near, beside)

            near = rbz[INDEX[s]]
            before = jnp.broadcast_to(to_col(rbe[4 + edge[(1, s)]], lane, row), near.shape)
            after = jnp.broadcast_to(to_col(rbe[4 + edge[(-1, s)]], lane, row), near.shape)
            full = jnp.where(lane == 0, before, near)
            full = jnp.where(lane == X + 1, after, full)
            beside = roll(near, -LANES, 1) + bz[INDEX[-s]] + roll(full, 1, 1) + roll(full, -1, 1)
            for t in SIGNS:
                beside = beside + yshift(near, t, rbe[8 + edge[(t, s)]])
            CZ[s] = chemical(near, beside)

        diffused = []
        for x in range(X):
            c = C[x]
            cy_up = yshift(c, -1, CY[-1][1 + x : 2 + x, :])
            cy_dn = yshift(c, 1, CY[1][1 + x : 2 + x, :])
            cz_up = zshift(c, -1, CZ[-1], 1 + x)
            cz_dn = zshift(c, 1, CZ[1], 1 + x)
            diffused.append(
                C[x + 1] + C[x - 1] + cy_up + cy_dn + cz_up + cz_dn - 6.0 * c
            )
            scale = -0.5 * O[x]
            force = [scale * (C[x + 1] - C[x - 1]), scale * (cy_up - cy_dn), scale * (cz_up - cz_dn)]
            rho, inv, u = moved[x]
            v = [u[d] + force[d] * inv for d in range(3)]
            flat = rho * (1.0 - 1.5 * (v[0] * v[0] + v[1] * v[1] + v[2] * v[2]))
            out = [None] * 19
            out[0] = post[0, x] + WEIGHTS[0] * flat
            for i in range(1, 19, 2):
                a = along(i, v)
                even = WEIGHTS[i] * flat + (4.5 * WEIGHTS[i]) * rho * (a * a)
                odd = (3.0 * WEIGHTS[i]) * rho * a
                out[i] = post[i, x] + even + odd
                out[i + 1] = post[i + 1, x] + even - odd
            for i in range(19):
                post[i, x] = out[i]
            for s in SIGNS:
                if x == (X - 1 if s == 1 else 0):
                    for slot, i in enumerate(CROSS[0][s]):
                        ax[INDEX[s], slot] = out[i]
                y = Y - 1 if s == 1 else 0
                for slot, i in enumerate(CROSS[1][s]):
                    ay[INDEX[s], slot, 1 + x : 2 + x, :] = out[i][y : y + 1, :]
        for s in SIGNS:
            az[INDEX[s]] = pack(
                [[(post[i, x], Z - 1 if s == 1 else 0) for x in range(X)] for i in CROSS[2][s]], s
            )

        messages = []
        for s in SIGNS:
            si = INDEX[s]
            messages.append((ax.at[si], rax.at[si], (s, 0, 0)))
            messages.append((ay.at[si], ray.at[si], (0, s, 0)))
            messages.append((az.at[si], raz.at[si], (0, 0, s)))
        for e, (a, b) in enumerate(EDGES):
            ae[e] = post[DIRS.index((a, b, 0)), xsrc(a)][ysrc(b) : ysrc(b) + 1, :]
            ae[4 + e] = to_row(post[DIRS.index((a, 0, b)), xsrc(a)], zsrc(b))
            i = DIRS.index((0, a, b))
            ae[8 + e] = corners([post[i, x] for x in range(X)], a, b)
            messages.append((ae.at[e], rae.at[e], (a, b, 0)))
            messages.append((ae.at[4 + e], rae.at[4 + e], (a, 0, b)))
            messages.append((ae.at[8 + e], rae.at[8 + e], (0, a, b)))
        finish(run(messages, sa, ra))

        flows = []
        for x in range(X):
            ps = []
            for i, (cx, cy, cz) in enumerate(DIRS):
                xs = x - cx
                own = 0 <= xs < X
                p = post[i, xs] if own else rax[INDEX[cx], CROSS[0][cx].index(i)]
                if cz:
                    at = CROSS[2][cz].index(i) * LANES + 1
                    if own:
                        p = zshift(p, cz, raz[INDEX[cz]], at + xs)
                    else:
                        p = zinsert(p, cz, to_col(rae[4 + edge[(cx, cz)]], lane, row), lane)
                if cy:
                    if own:
                        halo = ray[INDEX[cy], CROSS[1][cy].index(i), 1 + xs : 2 + xs, :]
                    else:
                        halo = rae[edge[(cx, cy)]]
                    if cz:
                        cell = roll(rae[8 + edge[(cy, cz)]], zend(cz) - (1 + x), 1)
                        halo = jnp.where(lane1 == zend(cz), cell, roll(halo, cz, 1))
                    p = yshift(p, cy, halo)
                pops[i, x] = p
                ps.append(p)
            rho, moms = moments(ps)
            inv = 1.0 / rho
            flows.append([m * inv for m in moms])

        for s in SIGNS:
            si = INDEX[s]
            y = Y - 1 if s == 1 else 0
            cx_[si] = flows[X - 1 if s == 1 else 0][0]
            for x in range(X):
                cy_[si, 1 + x : 2 + x, :] = flows[x][1][y : y + 1, :]
            cz_[si] = pack([[(flows[x][2], Z - 1 if s == 1 else 0) for x in range(X)]], s)
        messages = []
        for s in SIGNS:
            si = INDEX[s]
            messages.append((cx_.at[si], rcx.at[si], (s, 0, 0)))
            messages.append((cy_.at[si], rcy.at[si], (0, s, 0)))
            messages.append((cz_.at[si], rcz.at[si], (0, 0, s)))
        finish(run(messages, sc, rc))

        for x in range(X):
            f, pair = flows[x], pairs[x]
            fx_up = flows[x + 1][0] if x + 1 < X else rcx[1]
            fx_dn = flows[x - 1][0] if x > 0 else rcx[0]
            change = (f[0] + fx_up) * pair[(0, -1)] - (f[0] + fx_dn) * pair[(0, 1)]
            for s in SIGNS:
                fy = yshift(f[1], s, rcy[INDEX[s], 1 + x : 2 + x, :])
                fz = zshift(f[2], s, rcz[INDEX[s]], 1 + x)
                part = (f[1] + fy) * pair[(1, s)] + (f[2] + fz) * pair[(2, s)]
                change = change - part if s == 1 else change + part
            order[x] = O[x] - (0.25 * change - mobility * diffused[x])
        return carry

    lax.fori_loop(0, ITERS, step, 0)


def on_device(sizes, order_param, density, velocity):
    X, Y, Z = order_param.shape
    f32 = jnp.float32
    plane, rows = (Y, Z), (8, Z)
    vmem = [
        (19, X, Y, Z),
        (2, 5) + plane, (2, 5) + rows, (2,) + plane,
        (2, 5) + plane, (2, 5) + rows, (2,) + plane,
        (12, 1, Z), (12, 1, Z),
        (2, 2) + rows, (2,) + plane,
        (2, 2) + plane, (2, 2) + rows, (2,) + plane,
        (12, 1, Z), (12, 1, Z),
        (2,) + plane, (2,) + rows, (2,) + plane,
        (2,) + plane, (2,) + rows, (2,) + plane,
    ]
    sems = [18, 18, 18, 18, 6, 6]
    spec = pl.BlockSpec(memory_space=pltpu.VMEM)
    return pl.pallas_call(
        functools.partial(kernel, sizes),
        out_shape=(
            jax.ShapeDtypeStruct((X, Y, Z), f32),
            jax.ShapeDtypeStruct((19, X, Y, Z), f32),
        ),
        in_specs=[spec] * 3,
        out_specs=(spec, spec),
        scratch_shapes=[pltpu.VMEM(s, f32) for s in vmem]
        + [pltpu.SemaphoreType.DMA((n,)) for n in sems],
        compiler_params=pltpu.CompilerParams(collective_id=0, has_side_effects=True),
    )(order_param, density, velocity)


def solution(mesh):
    sizes = tuple(mesh.shape[a] for a in ("gx", "gy", "gz"))
    return jax.shard_map(
        functools.partial(on_device, sizes),
        mesh=mesh,
        in_specs=(P("gx", "gy", "gz"), P("gx", "gy", "gz"), P(None, "gx", "gy", "gz")),
        out_specs=(P("gx", "gy", "gz"), P(None, "gx", "gy", "gz")),
        check_vma=False,
    )
```

```python
import functools

import jax
import jax.numpy as jnp
from jax import lax
from jax.experimental import pallas as pl
from jax.experimental.pallas import tpu as pltpu
from jax.sharding import PartitionSpec as P

ITERS = 5
MESH = pl.DeviceIdType.MESH
DIRS = [
    (0, 0, 0),
    (1, 0, 0),
    (-1, 0, 0),
    (0, 1, 0),
    (0, -1, 0),
    (0, 0, 1),
    (0, 0, -1),
    (1, 1, 0),
    (-1, -1, 0),
    (1, -1, 0),
    (-1, 1, 0),
    (1, 0, 1),
    (-1, 0, -1),
    (1, 0, -1),
    (-1, 0, 1),
    (0, 1, 1),
    (0, -1, -1),
    (0, 1, -1),
    (0, -1, 1),
]
WEIGHTS = [1.0 / 3.0] + [1.0 / 18.0] * 6 + [1.0 / 36.0] * 12
quadratic = -0.1
quartic = 0.1
stiffness = 0.02
mobility = 0.5
relax_time = 0.8

SIGNS = (1, -1)
INDEX = {1: 0, -1: 1}
CROSS = [{s: [i for i in range(19) if DIRS[i][d] == s] for s in SIGNS} for d in range(3)]
EDGES = [(a, b) for a in SIGNS for b in SIGNS]
LANES = 8


def neighbours():
    out = []
    for d in range(3):
        for s in SIGNS:
            out.append(tuple(s if k == d else 0 for k in range(3)))
    out += [(a, b, 0) for a, b in EDGES]
    out += [(a, 0, b) for a, b in EDGES]
    out += [(0, a, b) for a, b in EDGES]
    return out


def kernel(sizes, order_in, dens_in, vel_in, order, pops, post, *scratch):
    (ax, ay, az, rax, ray, raz, ae, rae) = scratch[0:8]
    (by, bz, rbx, rby, rbz, be, rbe) = scratch[8:15]
    (cx_, cy_, cz_, rcx, rcy, rcz) = scratch[15:21]
    (sa, ra, sb, rb, sc, rc) = scratch[21:27]
    X, Y, Z = order.shape
    me = [lax.axis_index(a) for a in ("gx", "gy", "gz")]

    def device(off):
        return {
            a: lax.rem(me[k] + (off[k] + sizes[k]), sizes[k]) if off[k] else me[k]
            for k, a in enumerate(("gx", "gy", "gz"))
        }

    barrier = pltpu.get_barrier_semaphore()
    for off in neighbours():
        pl.semaphore_signal(barrier, inc=1, device_id=device(off), device_id_type=MESH)

    lane = lax.broadcasted_iota(jnp.int32, (Y, Z), 1)
    row = lax.broadcasted_iota(jnp.int32, (Y, Z), 0)
    lane8 = lax.broadcasted_iota(jnp.int32, (8, Z), 1)
    row8 = lax.broadcasted_iota(jnp.int32, (8, Z), 0)
    lane1 = lax.broadcasted_iota(jnp.int32, (1, Z), 1)

    def roll(v, s, axis):
        s = s % v.shape[axis]
        return v if s == 0 else pltpu.roll(v, s, axis)

    def zend(s):
        return 0 if s == 1 else Z - 1

    def yend(s):
        return 0 if s == 1 else Y - 1

    def zshift(v, s, packed, at):
        col = roll(packed, zend(s) - at, 1)
        return jnp.where(lane == zend(s), col, roll(v, s, 1))

    def yshift(v, s, halo):
        return jnp.where(row == yend(s), jnp.broadcast_to(halo, v.shape), roll(v, s, 0))

    def zinsert(v, s, col, lanes):
        return jnp.where(lanes == zend(s), jnp.broadcast_to(col, v.shape), roll(v, s, 1))

    def to_row(v, z):
        col = jnp.broadcast_to(v[:, z : z + 1], v.shape)
        return jnp.sum(jnp.where(lane == row, col, 0.0), axis=0, keepdims=True)

    def to_col(v, lanes, rows):
        v = jnp.broadcast_to(v, lanes.shape)
        return jnp.sum(jnp.where(lanes == rows, v, 0.0), axis=1, keepdims=True)

    def xsrc(s):
        return X - 1 if s == 1 else 0

    def ysrc(s):
        return Y - 1 if s == 1 else 0

    def zsrc(s):
        return Z - 1 if s == 1 else 0

    def corners(planes, b, c):
        y, acc = ysrc(b), jnp.zeros((1, Z), jnp.float32)
        for x in range(X):
            cells = roll(planes[x][y : y + 1, :], 1 + x - zsrc(c), 1)
            acc = jnp.where(lane1 == 1 + x, cells, acc)
        return acc

    def pack(fields, s):
        acc = jnp.zeros((Y, Z), jnp.float32)
        for slot, planes in enumerate(fields):
            for x in range(X):
                at = slot * LANES + 1 + x
                depth_lane = planes[x][1]
                acc = jnp.where(lane == at, roll(planes[x][0], at - depth_lane, 1), acc)
        return acc

    def run(messages, ssem, rsem, first=0):
        copies = []
        messages = sorted(messages, key=lambda m: (m[2][1] == 0, -sum(map(abs, m[2]))))
        for k, (src, dst, off) in enumerate(messages, first):
            copy = pltpu.make_async_remote_copy(
                src_ref=src,
                dst_ref=dst,
                send_sem=ssem.at[k],
                recv_sem=rsem.at[k],
                device_id=device(off),
                device_id_type=MESH,
            )
            copy.start()
            copies.append(copy)
        return copies

    def finish(copies):
        for copy in copies:
            copy.wait_recv()
        for copy in copies:
            copy.wait_send()

    for ref in (ay, by, cy_):
        ref[...] = jnp.zeros_like(ref)

    for x in range(X):
        order[x] = order_in[x]
        r = dens_in[x]
        u = [vel_in[d, x] for d in range(3)]
        usq = 1.0 - 1.5 * (u[0] * u[0] + u[1] * u[1] + u[2] * u[2])
        for i in range(19):
            along = None
            for d in range(3):
                if DIRS[i][d]:
                    t = u[d] if DIRS[i][d] == 1 else -u[d]
                    along = t if along is None else along + t
            if along is None:
                pops[i, x] = WEIGHTS[i] * r * usq
            else:
                pops[i, x] = WEIGHTS[i] * r * (usq + 3.0 * along + 4.5 * along * along)
    pl.semaphore_wait(barrier, len(neighbours()))

    outer_first = sorted(range(X), key=lambda x: (min(x, X - 1 - x), x))

    def moments(ps):
        rho = ps[0]
        for i in range(1, 19):
            rho = rho + ps[i]
        moms = []
        for d in range(3):
            up = functools.reduce(lambda a, b: a + b, [ps[i] for i in CROSS[d][1]])
            down = functools.reduce(lambda a, b: a + b, [ps[i] for i in CROSS[d][-1]])
            moms.append(up - down)
        return rho, moms

    def chemical(o, beside):
        return quadratic * o + quartic * o * o * o - stiffness * (beside - 6.0 * o)

    def step(_, carry):
        O = [order[x] for x in range(X)]
        for s in SIGNS:
            si = INDEX[s]
            for depth in range(2):
                y = Y - 1 - depth if s == 1 else depth
                for x in range(X):
                    by[si, depth, 1 + x : 2 + x, :] = O[x][y : y + 1, :]
        messages = []
        for s in SIGNS:
            si = INDEX[s]
            planes = order.at[pl.ds(X - 2, 2)] if s == 1 else order.at[pl.ds(0, 2)]
            messages.append((planes, rbx.at[si], (s, 0, 0)))
            messages.append((by.at[si], rby.at[si], (0, s, 0)))
        for e, (a, b) in enumerate(EDGES):
            be[e] = O[xsrc(a)][ysrc(b) : ysrc(b) + 1, :]
            be[4 + e] = to_row(O[xsrc(a)], zsrc(b))
            be[8 + e] = corners(O, a, b)
            messages.append((be.at[e], rbe.at[e], (a, b, 0)))
            messages.append((be.at[4 + e], rbe.at[4 + e], (a, 0, b)))
            messages.append((be.at[8 + e], rbe.at[8 + e], (0, a, b)))
        flying = run(messages, sb, rb)
        messages = []
        for s in SIGNS:
            si = INDEX[s]
            bz[si] = pack(
                [
                    [(O[x], Z - 1 - depth if s == 1 else depth) for x in range(X)]
                    for depth in range(2)
                ],
                s,
            )
            messages.append((bz.at[si], rbz.at[si], (0, 0, s)))
        flying = flying + run(messages, sb, rb, len(flying))

        keep = 1.0 - 1.0 / relax_time
        mix = 1.0 / relax_time - 1.0

        def along(i, w):
            a = None
            for d in range(3):
                if DIRS[i][d]:
                    t = w[d] if DIRS[i][d] == 1 else -w[d]
                    a = t if a is None else a + t
            return a

        moved = []
        for x in range(X):
            ps = [pops[i, x] for i in range(19)]
            rho, moms = moments(ps)
            inv = 1.0 / rho
            u = [m * inv for m in moms]
            flat = (mix * rho) * (1.0 - 1.5 * (u[0] * u[0] + u[1] * u[1] + u[2] * u[2]))
            post[0, x] = keep * ps[0] + WEIGHTS[0] * flat
            for i in range(1, 19, 2):
                a = along(i, u)
                even = WEIGHTS[i] * flat + (4.5 * mix * WEIGHTS[i]) * rho * (a * a)
                odd = (3.0 * mix * WEIGHTS[i]) * rho * a
                post[i, x] = keep * ps[i] + even + odd
                post[i + 1, x] = keep * ps[i + 1] + even - odd
            moved.append((rho, inv, u))
        finish(flying)

        edge = {ab: e for e, ab in enumerate(EDGES)}
        OX = {-2: rbx[0, 0], -1: rbx[0, 1], X: rbx[1, 0], X + 1: rbx[1, 1]}
        for x in range(X):
            OX[x] = O[x]

        def order_y(x, s):
            return yshift(O[x], s, rby[INDEX[s], 0, 1 + x : 2 + x, :])

        def order_z(x, s):
            return zshift(O[x], s, rbz[INDEX[s]], 1 + x)

        C, pairs = {}, []
        for x in range(X):
            near = {(0, 1): OX[x - 1], (0, -1): OX[x + 1]}
            for s in SIGNS:
                near[(1, s)], near[(2, s)] = order_y(x, s), order_z(x, s)
            C[x] = chemical(O[x], functools.reduce(lambda a, b: a + b, near.values()))
            pairs.append({k: O[x] + v for k, v in near.items()})
        for s in SIGNS:
            x = -1 if s == 1 else X
            p = OX[x]
            beside = OX[x - 1] + OX[x + 1]
            for t in SIGNS:
                e = edge[(s, t)]
                beside = beside + yshift(p, t, rbe[e])
                beside = beside + zinsert(p, t, to_col(rbe[4 + e], lane, row), lane)
            C[x] = chemical(p, beside)
        CY, CZ = {}, {}
        for s in SIGNS:
            near = rby[INDEX[s], 0]
            full = jnp.where(row8 == 0, jnp.broadcast_to(rbe[edge[(1, s)]], near.shape), near)
            after = jnp.broadcast_to(rbe[edge[(-1, s)]], near.shape)
            full = jnp.where(row8 == X + 1, after, full)
            beside = rby[INDEX[s], 1] + by[INDEX[-s], 0] + roll(full, 1, 0) + roll(full, -1, 0)
            for t in SIGNS:
                col = to_col(rbe[8 + edge[(s, t)]], lane8, row8)
                beside = beside + zinsert(near, t, col, lane8)
            CY[s] = chemical(near, beside)

            near = rbz[INDEX[s]]
            before = jnp.broadcast_to(to_col(rbe[4 + edge[(1, s)]], lane, row), near.shape)
            after = jnp.broadcast_to(to_col(rbe[4 + edge[(-1, s)]], lane, row), near.shape)
            full = jnp.where(lane == 0, before, near)
            full = jnp.where(lane == X + 1, after, full)
            beside = roll(near, -LANES, 1) + bz[INDEX[-s]] + roll(full, 1, 1) + roll(full, -1, 1)
            for t in SIGNS:
                beside = beside + yshift(near, t, rbe[8 + edge[(t, s)]])
            CZ[s] = chemical(near, beside)

        diffused = {}
        flying = []
        for place, x in enumerate(outer_first):
            c = C[x]
            cy_up = yshift(c, -1, CY[-1][1 + x : 2 + x, :])
            cy_dn = yshift(c, 1, CY[1][1 + x : 2 + x, :])
            cz_up = zshift(c, -1, CZ[-1], 1 + x)
            cz_dn = zshift(c, 1, CZ[1], 1 + x)
            diffused[x] = C[x + 1] + C[x - 1] + cy_up + cy_dn + cz_up + cz_dn - 6.0 * c
            scale = -0.5 * O[x]
            force = [scale * (C[x + 1] - C[x - 1]), scale * (cy_up - cy_dn), scale * (cz_up - cz_dn)]
            rho, inv, u = moved[x]
            v = [u[d] + force[d] * inv for d in range(3)]
            flat = rho * (1.0 - 1.5 * (v[0] * v[0] + v[1] * v[1] + v[2] * v[2]))
            out = [None] * 19
            out[0] = post[0, x] + WEIGHTS[0] * flat
            for i in range(1, 19, 2):
                a = along(i, v)
                even = WEIGHTS[i] * flat + (4.5 * WEIGHTS[i]) * rho * (a * a)
                odd = (3.0 * WEIGHTS[i]) * rho * a
                out[i] = post[i, x] + even + odd
                out[i + 1] = post[i + 1, x] + even - odd
            for i in range(19):
                post[i, x] = out[i]
            for s in SIGNS:
                if x == (X - 1 if s == 1 else 0):
                    for slot, i in enumerate(CROSS[0][s]):
                        ax[INDEX[s], slot] = out[i]
                y = Y - 1 if s == 1 else 0
                for slot, i in enumerate(CROSS[1][s]):
                    ay[INDEX[s], slot, 1 + x : 2 + x, :] = out[i][y : y + 1, :]
            if place == 1:
                early = []
                for s in SIGNS:
                    early.append((ax.at[INDEX[s]], rax.at[INDEX[s]], (s, 0, 0)))
                for e, (a, b) in enumerate(EDGES):
                    ae[e] = post[DIRS.index((a, b, 0)), xsrc(a)][ysrc(b) : ysrc(b) + 1, :]
                    ae[4 + e] = to_row(post[DIRS.index((a, 0, b)), xsrc(a)], zsrc(b))
                    early.append((ae.at[e], rae.at[e], (a, b, 0)))
                    early.append((ae.at[4 + e], rae.at[4 + e], (a, 0, b)))
                flying = run(early, sa, ra)

        messages = []
        for e, (a, b) in enumerate(EDGES):
            i = DIRS.index((0, a, b))
            ae[8 + e] = corners([post[i, x] for x in range(X)], a, b)
            messages.append((ae.at[8 + e], rae.at[8 + e], (0, a, b)))
        for s in SIGNS:
            messages.append((ay.at[INDEX[s]], ray.at[INDEX[s]], (0, s, 0)))
        flying = flying + run(messages, sa, ra, len(flying))
        messages = []
        for s in SIGNS:
            az[INDEX[s]] = pack(
                [[(post[i, x], Z - 1 if s == 1 else 0) for x in range(X)] for i in CROSS[2][s]], s
            )
            messages.append((az.at[INDEX[s]], raz.at[INDEX[s]], (0, 0, s)))
        flying = flying + run(messages, sa, ra, len(flying))
        finish(flying)

        flows = {}
        flying = []
        for place, x in enumerate(outer_first):
            ps = []
            for i, (cx, cy, cz) in enumerate(DIRS):
                xs = x - cx
                own = 0 <= xs < X
                p = post[i, xs] if own else rax[INDEX[cx], CROSS[0][cx].index(i)]
                if cz:
                    at = CROSS[2][cz].index(i) * LANES + 1
                    if own:
                        p = zshift(p, cz, raz[INDEX[cz]], at + xs)
                    else:
                        p = zinsert(p, cz, to_col(rae[4 + edge[(cx, cz)]], lane, row), lane)
                if cy:
                    if own:
                        halo = ray[INDEX[cy], CROSS[1][cy].index(i), 1 + xs : 2 + xs, :]
                    else:
                        halo = rae[edge[(cx, cy)]]
                    if cz:
                        cell = roll(rae[8 + edge[(cy, cz)]], zend(cz) - (1 + x), 1)
                        halo = jnp.where(lane1 == zend(cz), cell, roll(halo, cz, 1))
                    p = yshift(p, cy, halo)
                pops[i, x] = p
                ps.append(p)
            rho, moms = moments(ps)
            inv = 1.0 / rho
            flows[x] = [m * inv for m in moms]
            if place == 1:
                early = []
                for s in SIGNS:
                    cx_[INDEX[s]] = flows[xsrc(s)][0]
                    early.append((cx_.at[INDEX[s]], rcx.at[INDEX[s]], (s, 0, 0)))
                flying = run(early, sc, rc)

        for s in SIGNS:
            si = INDEX[s]
            y = Y - 1 if s == 1 else 0
            for x in range(X):
                cy_[si, 1 + x : 2 + x, :] = flows[x][1][y : y + 1, :]
            cz_[si] = pack([[(flows[x][2], Z - 1 if s == 1 else 0) for x in range(X)]], s)
        messages = []
        for s in SIGNS:
            si = INDEX[s]
            messages.append((cy_.at[si], rcy.at[si], (0, s, 0)))
            messages.append((cz_.at[si], rcz.at[si], (0, 0, s)))
        finish(flying + run(messages, sc, rc, len(flying)))

        for x in range(X):
            f, pair = flows[x], pairs[x]
            fx_up = flows[x + 1][0] if x + 1 < X else rcx[1]
            fx_dn = flows[x - 1][0] if x > 0 else rcx[0]
            change = (f[0] + fx_up) * pair[(0, -1)] - (f[0] + fx_dn) * pair[(0, 1)]
            for s in SIGNS:
                fy = yshift(f[1], s, rcy[INDEX[s], 1 + x : 2 + x, :])
                fz = zshift(f[2], s, rcz[INDEX[s]], 1 + x)
                part = (f[1] + fy) * pair[(1, s)] + (f[2] + fz) * pair[(2, s)]
                change = change - part if s == 1 else change + part
            order[x] = O[x] - (0.25 * change - mobility * diffused[x])
        return carry

    lax.fori_loop(0, ITERS, step, 0)


def on_device(sizes, order_param, density, velocity):
    X, Y, Z = order_param.shape
    f32 = jnp.float32
    plane, rows = (Y, Z), (8, Z)
    vmem = [
        (19, X, Y, Z),
        (2, 5) + plane, (2, 5) + rows, (2,) + plane,
        (2, 5) + plane, (2, 5) + rows, (2,) + plane,
        (12, 1, Z), (12, 1, Z),
        (2, 2) + rows, (2,) + plane,
        (2, 2) + plane, (2, 2) + rows, (2,) + plane,
        (12, 1, Z), (12, 1, Z),
        (2,) + plane, (2,) + rows, (2,) + plane,
        (2,) + plane, (2,) + rows, (2,) + plane,
    ]
    sems = [18, 18, 18, 18, 6, 6]
    spec = pl.BlockSpec(memory_space=pltpu.VMEM)
    return pl.pallas_call(
        functools.partial(kernel, sizes),
        out_shape=(
            jax.ShapeDtypeStruct((X, Y, Z), f32),
            jax.ShapeDtypeStruct((19, X, Y, Z), f32),
        ),
        in_specs=[spec] * 3,
        out_specs=(spec, spec),
        scratch_shapes=[pltpu.VMEM(s, f32) for s in vmem]
        + [pltpu.SemaphoreType.DMA((n,)) for n in sems],
        compiler_params=pltpu.CompilerParams(collective_id=0, has_side_effects=True),
    )(order_param, density, velocity)


def solution(mesh):
    sizes = tuple(mesh.shape[a] for a in ("gx", "gy", "gz"))
    return jax.shard_map(
        functools.partial(on_device, sizes),
        mesh=mesh,
        in_specs=(P("gx", "gy", "gz"), P("gx", "gy", "gz"), P(None, "gx", "gy", "gz")),
        out_specs=(P("gx", "gy", "gz"), P(None, "gx", "gy", "gz")),
        check_vma=False,
    )
```
